128 devices in a mesh: rows: 16 (over z, x), cols: 8 (over y, core).
Axes of the slice: x: 4, y: 4, z: 4, core: 2. Of those that a mesh axis runs over, the one named last changes fastest.
Arguments:
- densities: bfloat16 [6, 8192, 128, 128], P(None, ('rows', 'cols')), may hold values from -6 to 6
- residuals: bfloat16 [6, 8192, 128, 128], P(None, ('rows', 'cols')), may hold values from -32 to 32
- block_pairs: int32 [2, 8192], P(None, ('rows', 'cols')), may hold values from 0 to 1562
- new_owner: int32 [8192], P(('rows', 'cols')), may hold values from -1 to 15, as said below
Outputs:
- owned_blocks: bfloat16 [4096, 128, 128], P(('rows', 'cols'))
- coefficients: float32 [6], replicated
The draws below stay inside these ranges and needn't reach their ends.
Inputs may be any that keep to these rules, and one draw needn't show every extreme that they name: A live block stays at its index of cols and moves to index new_owner of rows. For each index of cols, every index of rows becomes the owner of exactly 32 blocks, and at most 4 of them come from one device.
All inputs are finite; a program needn't handle non-finite values.
Results may differ from the reference program's by a relative error of at most 0.0019.
Values may be sent and summed in bfloat16 or wider, within the bound.
A program may use at most 128 MiB of HBM per device.

```python
import jax
import jax.numpy as jnp
from jax import lax

BLOCK = 128
ROW_BLOCKS = 1563
HISTORY = 5
OWNED = 32
HELD = 64
SLOTS = 8192
N_ROWS = 16
N_COLS = 8


def draw_residuals(key, part):
    full_shape = (HISTORY + 1, SLOTS, BLOCK, BLOCK)
    key_noise = jax.random.fold_in(key, 0)
    key_scale = jax.random.fold_in(key, 1)
    key_history = jax.random.fold_in(key, 4)
    key_lines = jax.random.fold_in(key, 5)
    key_across = jax.random.fold_in(key, 6)
    device_of = jnp.arange(SLOTS, dtype=jnp.int32) // HELD
    device_count = SLOTS // HELD
    ramp_scale = 1.0 + device_of.astype(jnp.float32) / max(device_count - 1, 1)
    history_scale = jnp.exp(jax.random.uniform(key_history, (HISTORY + 1, SLOTS), jnp.float32, jnp.log(0.35), jnp.log(2.8)))
    line_factor = jnp.exp(jax.random.uniform(key_lines, (HISTORY + 1, 1, BLOCK, 1), jnp.float32, jnp.log(0.1), jnp.log(10.0)))
    across_factor = jnp.exp(jax.random.uniform(key_across, (HISTORY + 1, 1, 1, BLOCK), jnp.float32, jnp.log(0.1), jnp.log(10.0)))
    values = jax.random.normal(key_noise, full_shape, jnp.float32)
    slot_scale = jnp.exp(jax.random.uniform(key_scale, (SLOTS,), jnp.float32, jnp.log(0.25), jnp.log(4.0)))
    values = values * (history_scale * (ramp_scale * slot_scale)[None, :])[:, :, None, None]
    values = 0.06 * values * line_factor * across_factor
    return jnp.clip(values, -32.0, 32.0).astype(jnp.bfloat16)


def draw_block_pairs(key, part):
    key_row, key_col, key_diag = jax.random.split(key, 3)
    row_ids = jax.random.randint(key_row, (SLOTS,), 0, ROW_BLOCKS, dtype=jnp.int32)
    col_ids = jax.random.randint(key_col, (SLOTS,), 0, ROW_BLOCKS, dtype=jnp.int32)
    diagonal = jax.random.randint(key_diag, (SLOTS,), 0, 2, dtype=jnp.int32) == 0
    return jnp.stack([row_ids, jnp.where(diagonal, row_ids, col_ids)]).astype(jnp.int32)


def draw_new_owner(key, part):
    rows_total = N_ROWS
    cols_total = SLOTS // HELD // N_ROWS
    pair_cap = HELD // rows_total
    key_pick, key_perm = jax.random.split(key, 2)
    picks = jax.random.randint(key_pick, (cols_total, rows_total // 4, rows_total), 1, 4, dtype=jnp.int32)
    row_ids = jnp.arange(rows_total, dtype=jnp.int32)
    picked_row = picks[:, row_ids // 4, :]
    sends = (row_ids % 4 == 0)[None, :, None] | ((row_ids % 4)[None, :, None] == picked_row)
    entry_ids = jnp.arange(HELD, dtype=jnp.int32)
    entry_owner = entry_ids // pair_cap
    values = jnp.where(sends[:, :, entry_owner], entry_owner[None, None, :], -1).astype(jnp.int32)
    scores = jax.random.randint(key_perm, (cols_total, rows_total, HELD), 0, 1 << 20, dtype=jnp.int32) * HELD + entry_ids
    orders = jnp.argsort(scores, axis=2, stable=True).astype(jnp.int32)
    column_ids = jnp.arange(cols_total, dtype=jnp.int32)[:, None, None]
    device_ids = row_ids[None, :, None] * cols_total + column_ids
    flat_slot = device_ids * HELD + orders
    return jnp.full((SLOTS,), -1, jnp.int32).at[flat_slot.reshape(-1)].set(values.reshape(-1))


def block_scale(stream_key, shape, shards, smallest, high):
    gain = 1.0
    for dim, blocks in shards:
        steps = jax.random.uniform(jax.random.fold_in(jax.random.fold_in(stream_key, 6), dim), (blocks,), jnp.float32, smallest / len(shards), high / len(shards))
        gain = gain * jnp.repeat(jnp.exp(steps), shape[dim] // blocks).reshape((-1,) + (1,) * (len(shape) - 1 - dim))
    return gain


def scatter_about(own_key, shape, spread, most, cuts=(), kind=jnp.bfloat16):
    level = block_scale(own_key, shape, cuts, -0.22, 0.18) if cuts else 1.0
    values = jax.random.normal(own_key, shape, jnp.float32) * spread * level
    return jnp.minimum(jnp.maximum(values, -most), most).astype(kind)


def setup_inputs(seed: int = 0) -> dict:
    key_list = jax.random.split(jax.random.key(seed), 5)
    densities = scatter_about(key_list[0], (HISTORY + 1, SLOTS, BLOCK, BLOCK), 1.0, 6.0, ((1, 128),))
    residuals = draw_residuals(jax.random.fold_in(key_list[4], 71), 0)
    block_pairs = draw_block_pairs(jax.random.fold_in(key_list[4], 71), 0)
    new_owner = draw_new_owner(jax.random.fold_in(key_list[4], 71), 0)
    return dict(densities=densities, residuals=residuals, block_pairs=block_pairs, new_owner=new_owner)


mix_weight = 0.3


def small_solve(system, vector):
    order_n = system.shape[0]
    positions = jnp.arange(order_n, dtype=jnp.int32)
    for step_index in range(order_n):
        column = system[:, step_index] / system[step_index, step_index]
        column = jnp.where(positions > step_index, column, 0.0)
        system = system - column[:, None] * system[step_index][None, :]
        vector = vector - column * vector[step_index]
    solution = jnp.zeros((order_n,), jnp.float32)
    for step_index in reversed(range(order_n)):
        inner = jnp.sum(jnp.where(positions > step_index, system[step_index] * solution, 0.0))
        solution = solution.at[step_index].set((vector[step_index] - inner) / system[step_index, step_index])
    return solution


def reference(densities, residuals, block_pairs, new_owner):
    slot_total = new_owner.shape[0]
    history_count = densities.shape[0]
    devices_all = N_ROWS * N_COLS
    alive_slot = new_owner >= 0
    slot_weight = jnp.where(alive_slot, jnp.where(block_pairs[0] == block_pairs[1], 1.0, 2.0), 0.0).astype(jnp.float32)

    def gram_step(running, device):
        first_slot = (device * HELD).astype(jnp.int32)
        residual_part = lax.dynamic_slice_in_dim(residuals, first_slot, HELD, 1).astype(jnp.float32)
        weight_part = lax.dynamic_slice_in_dim(slot_weight, first_slot, HELD, 0)
        per_slot = jnp.einsum("isxy,ksxy->sik", residual_part, residual_part, precision=lax.Precision.HIGHEST)
        return running + jnp.einsum("s,sik->ik", weight_part, per_slot, precision=lax.Precision.HIGHEST), None

    correlation = lax.scan(gram_step, jnp.zeros((history_count, history_count), jnp.float32), jnp.arange(devices_all, dtype=jnp.int32))[0]
    solved = small_solve(correlation, jnp.ones((history_count,), jnp.float32))
    coefficients = solved / jnp.sum(solved)

    def blend_step(device):
        first_slot = (device * HELD).astype(jnp.int32)
        density_part = lax.dynamic_slice_in_dim(densities, first_slot, HELD, 1)
        residual_part = lax.dynamic_slice_in_dim(residuals, first_slot, HELD, 1)
        running = jnp.zeros(density_part.shape[1:], jnp.float32)
        for hist_index in range(history_count):
            running = running + coefficients[hist_index] * (density_part[hist_index].astype(jnp.float32) + mix_weight * residual_part[hist_index].astype(jnp.float32))
        return running.astype(jnp.bfloat16)

    mixed_blocks = lax.map(blend_step, jnp.arange(devices_all, dtype=jnp.int32)).reshape(slot_total, BLOCK, BLOCK)
    slot_ids = jnp.arange(slot_total, dtype=jnp.int32)
    column_of = (slot_ids // HELD) % N_COLS
    destination = jnp.where(alive_slot, new_owner * N_COLS + column_of, devices_all).astype(jnp.int32)
    onehot = (destination[:, None] == jnp.arange(devices_all, dtype=jnp.int32)[None, :]).astype(jnp.int32)
    ranking = jnp.sum(jnp.cumsum(onehot, axis=0) * onehot, axis=1) - 1
    target_slot = jnp.where(alive_slot, destination * OWNED + ranking, devices_all * OWNED).astype(jnp.int32)
    owned_blocks = jnp.zeros((devices_all * OWNED, BLOCK, BLOCK), jnp.bfloat16).at[target_slot].set(mixed_blocks, mode="drop")
    return owned_blocks, coefficients
```

```python
import functools

import jax
import jax.numpy as jnp
from jax import lax
from jax.experimental import pallas as pl
from jax.experimental.pallas import tpu as pltpu
from jax.sharding import PartitionSpec as P

MESH = pl.DeviceIdType.MESH

HIST = 6
HELD = 64
OWNED = 32
BLOCK = 128
CAP = 4
CHUNK = 4
N_CHUNKS = HELD // CHUNK
GROUP = 32
STACK = HIST * GROUP

mix_weight = 0.3


def kernel(
    n_rows,
    n_cols,
    dens_hbm,
    res_hbm,
    pairs,
    owner,
    owner_row,
    owned,
    coef_out,
    dens,
    res,
    acc,
    outgoing,
    arrived,
    cols_in,
    rows_in,
    cols_out,
    rows_out,
    counts_in,
    counts_out,
    table_v,
    table_s,
    order_v,
    order_s,
    res_sem,
    dens_sem,
    cols_send,
    cols_recv,
    rows_send,
    rows_recv,
    counts_send,
    counts_recv,
    move_send,
    move_recv,
    table_sem,
):
    my_row = lax.axis_index("rows")
    my_col = lax.axis_index("cols")

    def chunk_copy(src, dst, sem, c):
        part = pl.ds(c * CHUNK, CHUNK)
        return pltpu.make_async_copy(src.at[:, part], dst.at[:, part], sem.at[c])

    for c in range(N_CHUNKS):
        chunk_copy(res_hbm, res, res_sem, c).start()

    row_peers = [lax.rem(my_row + o, n_rows) for o in range(1, n_rows)]
    col_peers = [lax.rem(my_col + o, n_cols) for o in range(1, n_cols)]

    barrier = pltpu.get_barrier_semaphore()
    for r in row_peers:
        pl.semaphore_signal(barrier, inc=1, device_id={"rows": r}, device_id_type=MESH)
    for c in col_peers:
        pl.semaphore_signal(barrier, inc=1, device_id={"cols": c}, device_id_type=MESH)

    own = jnp.broadcast_to(owner_row[...], (HELD, HELD))
    down = lax.broadcasted_iota(jnp.int32, (HELD, HELD), 0)
    across = lax.broadcasted_iota(jnp.int32, (HELD, HELD), 1)
    own_down = jnp.sum(jnp.where(down == across, own, 0), axis=1, keepdims=True)
    same_before = (own == own_down) & (across < down)
    rank_down = jnp.sum(jnp.where(same_before, 1, 0), axis=1, keepdims=True)
    place_down = jnp.where(own_down >= 0, own_down * CAP + rank_down, -1)
    table_v[...] = jnp.sum(jnp.where(place_down == across, down, 0), axis=0, keepdims=True)
    lanes = lax.broadcasted_iota(jnp.int32, (HELD, BLOCK), 1)
    counts_out[...] = jnp.sum(jnp.where(own_down == lanes, 1, 0), axis=0, keepdims=True)
    table_copy = pltpu.make_async_copy(table_v, table_s, table_sem.at[0])
    table_copy.start()

    acc[...] = jnp.zeros_like(acc)

    def gram_slot(s):
        live = owner[s] >= 0
        weight = jnp.where(live, jnp.where(pairs[0, s] == pairs[1, s], 1.0, 2.0), 0.0)
        parts = [
            res[:, s, pl.ds(g * GROUP, GROUP), :].reshape(STACK, BLOCK)
            for g in range(BLOCK // GROUP)
        ]
        left = jnp.concatenate(parts, axis=1)
        return left, left * weight.astype(jnp.bfloat16)

    def gram_chunk(c, carry):
        chunk_copy(res_hbm, res, res_sem, c).wait()
        chunk_copy(dens_hbm, dens, dens_sem, c).start()
        for h in range(CHUNK // 2):
            pieces = [gram_slot(c * CHUNK + h * 2 + j) for j in range(2)]
            left = jnp.concatenate([p[0] for p in pieces], axis=1)
            right = jnp.concatenate([p[1] for p in pieces], axis=1)
            acc[...] += lax.dot_general(
                left, right, (((1,), (1,)), ((), ())), preferred_element_type=jnp.float32
            )
        return carry

    lax.fori_loop(0, N_CHUNKS, gram_chunk, 0)

    x_down = lax.broadcasted_iota(jnp.int32, (STACK, STACK), 0)
    x_across = lax.broadcasted_iota(jnp.int32, (STACK, STACK), 1)
    same_x = lax.rem(x_down, GROUP) == lax.rem(x_across, GROUP)
    diag = jnp.where(same_x, acc[...], 0.0).reshape(HIST, GROUP, STACK)
    by_iterate = jnp.sum(diag, axis=1)
    seg = lax.broadcasted_iota(jnp.int32, (HIST, STACK), 1) // GROUP
    i_at = lax.broadcasted_iota(jnp.int32, (HIST, BLOCK), 0)
    lane_at = lax.broadcasted_iota(jnp.int32, (HIST, BLOCK), 1)
    packed = jnp.zeros((HIST, BLOCK), jnp.float32)
    for k in range(HIST):
        entry = jnp.sum(jnp.where(seg == k, by_iterate, 0.0), axis=1, keepdims=True)
        packed = jnp.where(lane_at == i_at * 8 + k, entry, packed)
    row = jnp.sum(packed, axis=0, keepdims=True)

    pl.semaphore_wait(barrier, n_rows + n_cols - 2)

    cols_out[...] = row
    cols_in[my_col] = row

    def cols_copy(peer, slot):
        return pltpu.make_async_remote_copy(
            src_ref=cols_out,
            dst_ref=cols_in.at[slot],
            send_sem=cols_send.at[peer],
            recv_sem=cols_recv.at[slot],
            device_id={"cols": peer},
            device_id_type=MESH,
        )

    def rows_copy(peer, slot):
        return pltpu.make_async_remote_copy(
            src_ref=rows_out,
            dst_ref=rows_in.at[slot],
            send_sem=rows_send.at[peer],
            recv_sem=rows_recv.at[slot],
            device_id={"rows": peer},
            device_id_type=MESH,
        )

    def counts_copy(peer, slot):
        return pltpu.make_async_remote_copy(
            src_ref=counts_out,
            dst_ref=counts_in.at[slot],
            send_sem=counts_send.at[peer],
            recv_sem=counts_recv.at[slot],
            device_id={"rows": peer},
            device_id_type=MESH,
        )

    def move_copy(peer, slot):
        return pltpu.make_async_remote_copy(
            src_ref=outgoing.at[peer],
            dst_ref=arrived.at[pl.ds(slot * CAP, CAP)],
            send_sem=move_send.at[peer],
            recv_sem=move_recv.at[slot],
            device_id={"rows": peer},
            device_id_type=MESH,
        )

    for c in col_peers:
        cols_copy(c, my_col).start()
    counts_in[my_row] = counts_out[...]
    for r in row_peers:
        counts_copy(r, my_row).start()
    for c in col_peers:
        cols_copy(c, c).wait_recv()
    row = jnp.sum(cols_in[...], axis=0)
    rows_out[...] = row
    rows_in[my_row] = row
    for r in row_peers:
        rows_copy(r, my_row).start()
    for c in range(N_CHUNKS):
        chunk_copy(dens_hbm, dens, dens_sem, c).wait()
    table_copy.wait()
    for r in row_peers:
        rows_copy(r, r).wait_recv()
    total = jnp.sum(rows_in[...], axis=0)

    def spread(i, k):
        return jnp.broadcast_to(total[:, i * 8 + k : i * 8 + k + 1], (8, BLOCK))

    a = {(i, k): spread(i, k) for i in range(HIST) for k in range(i, HIST)}
    b = [jnp.ones((8, BLOCK), jnp.float32) for _ in range(HIST)]
    for j in range(HIST):
        for i in range(j + 1, HIST):
            factor = a[j, i] / a[j, j]
            for k in range(i, HIST):
                a[i, k] = a[i, k] - factor * a[j, k]
            b[i] = b[i] - factor * b[j]
    solved = [None] * HIST
    for j in reversed(range(HIST)):
        inner = b[j]
        for k in range(j + 1, HIST):
            inner = inner - a[j, k] * solved[k]
        solved[j] = inner / a[j, j]
    norm = functools.reduce(lambda p, q: p + q, solved)
    coef = [s / norm for s in solved]
    lane = lax.broadcasted_iota(jnp.int32, (8, BLOCK), 1)
    shown = jnp.zeros((8, BLOCK), jnp.float32)
    for i in range(HIST):
        shown = jnp.where(lane == i, coef[i], shown)
    coef_out[...] = shown

    coef_d = [c[0:1, :] for c in coef]
    coef_r = [c[0:1, :] * mix_weight for c in coef]

    def blend(q, k):
        slot = table_s[0, q * CAP + k]
        running = None
        for i in range(HIST):
            term = coef_d[i] * dens[i, slot].astype(jnp.float32)
            running = term if running is None else running + term
            running = running + coef_r[i] * res[i, slot].astype(jnp.float32)
        return running.astype(jnp.bfloat16)

    def send_step(o, carry):
        q = lax.rem(my_row + o, n_rows)
        for k in range(CAP):
            outgoing[q, k] = blend(q, k)
        move_copy(q, my_row).start()
        return carry

    lax.fori_loop(1, n_rows, send_step, 0)
    for k in range(CAP):
        arrived[my_row * CAP + k] = blend(my_row, k)

    for r in row_peers:
        counts_copy(r, r).wait_recv()
    counts = counts_in[...].reshape(n_rows, BLOCK)
    lanes = lax.broadcasted_iota(jnp.int32, (n_rows, BLOCK), 1)
    count_down = jnp.sum(jnp.where(lanes == my_row, counts, 0), axis=1, keepdims=True)
    row_down = lax.broadcasted_iota(jnp.int32, (n_rows, BLOCK), 0)
    count_across = jnp.sum(
        jnp.where(lanes == row_down, count_down, 0), axis=0, keepdims=True
    )
    upto_down = jnp.sum(
        jnp.where(lanes <= row_down, count_across, 0), axis=1, keepdims=True
    )
    skipped = jnp.sum(
        jnp.where(upto_down <= lanes, CAP - count_down, 0), axis=0, keepdims=True
    )
    place = lax.broadcasted_iota(jnp.int32, (1, BLOCK), 1)
    order_v[...] = jnp.minimum(place + skipped, n_rows * CAP - 1)
    order_copy = pltpu.make_async_copy(order_v, order_s, table_sem.at[1])
    order_copy.start()
    order_copy.wait()

    for r in row_peers:
        move_copy(r, r).wait_recv()

    def keep(p, carry):
        owned[p] = arrived[order_s[0, p]]
        return carry

    lax.fori_loop(0, OWNED, keep, 0)

    for c in col_peers:
        cols_copy(c, my_col).wait_send()
    for r in row_peers:
        counts_copy(r, my_row).wait_send()
        rows_copy(r, my_row).wait_send()
        move_copy(r, my_row).wait_send()


def solution(mesh):
    n_rows, n_cols = mesh.shape["rows"], mesh.shape["cols"]

    def on_device(densities, residuals, block_pairs, new_owner):
        vmem = pltpu.VMEM
        dma = pltpu.SemaphoreType.DMA
        owned, coef = pl.pallas_call(
            functools.partial(kernel, n_rows, n_cols),
            out_shape=(
                jax.ShapeDtypeStruct((OWNED, BLOCK, BLOCK), jnp.bfloat16),
                jax.ShapeDtypeStruct((8, BLOCK), jnp.float32),
            ),
            in_specs=[
                pl.BlockSpec(memory_space=pl.ANY),
                pl.BlockSpec(memory_space=pl.ANY),
                pl.BlockSpec(memory_space=pltpu.SMEM),
                pl.BlockSpec(memory_space=pltpu.SMEM),
                pl.BlockSpec(memory_space=pltpu.VMEM),
            ],
            out_specs=(
                pl.BlockSpec(memory_space=pltpu.VMEM),
                pl.BlockSpec(memory_space=pltpu.VMEM),
            ),
            scratch_shapes=[
                vmem((HIST, HELD, BLOCK, BLOCK), jnp.bfloat16),
                vmem((HIST, HELD, BLOCK, BLOCK), jnp.bfloat16),
                vmem((STACK, STACK), jnp.float32),
                vmem((n_rows, CAP, BLOCK, BLOCK), jnp.bfloat16),
                vmem((n_rows * CAP, BLOCK, BLOCK), jnp.bfloat16),
                vmem((n_cols, 1, BLOCK), jnp.float32),
                vmem((n_rows, 1, BLOCK), jnp.float32),
                vmem((1, BLOCK), jnp.float32),
                vmem((1, BLOCK), jnp.float32),
                vmem((n_rows, 1, BLOCK), jnp.int32),
                vmem((1, BLOCK), jnp.int32),
                vmem((1, HELD), jnp.int32),
                pltpu.SMEM((1, HELD), jnp.int32),
                vmem((1, BLOCK), jnp.int32),
                pltpu.SMEM((1, BLOCK), jnp.int32),
                dma((N_CHUNKS,)),
                dma((N_CHUNKS,)),
                dma((n_cols,)),
                dma((n_cols,)),
                dma((n_rows,)),
                dma((n_rows,)),
                dma((n_rows,)),
                dma((n_rows,)),
                dma((n_rows,)),
                dma((n_rows,)),
                dma((2,)),
            ],
            compiler_params=pltpu.CompilerParams(
                collective_id=0, has_side_effects=True, vmem_limit_bytes=48 * 1024 * 1024
            ),
        )(densities, residuals, block_pairs, new_owner, new_owner.reshape(1, HELD))
        return owned, coef[0, :HIST]

    placed = P(None, ("rows", "cols"), None, None)
    return jax.shard_map(
        on_device,
        mesh=mesh,
        in_specs=(placed, placed, P(None, ("rows", "cols")), P(("rows", "cols"))),
        out_specs=(P(("rows", "cols"), None, None), P()),
        check_vma=False,
    )
```

```python
import functools

import jax
import jax.numpy as jnp
from jax import lax
from jax.experimental import pallas as pl
from jax.experimental.pallas import tpu as pltpu
from jax.sharding import PartitionSpec as P

MESH = pl.DeviceIdType.MESH

HIST = 6
HELD = 64
OWNED = 32
BLOCK = 128
CAP = 4
CHUNK = 8
N_CHUNKS = HELD // CHUNK
GROUP = 32
STACK = HIST * GROUP
SEND_ORDER = [10, 6, 14, 9, 11, 2, 5, 15, 7, 13, 8, 1, 3, 4, 12]

mix_weight = 0.3


def kernel(
    n_rows,
    n_cols,
    dens_hbm,
    res_hbm,
    pairs_hbm,
    owner_hbm,
    owned,
    coef_out,
    pairs,
    owner,
    owner_row,
    dens,
    res,
    acc,
    outgoing,
    arrived,
    cols_in,
    rows_in,
    cols_out,
    rows_out,
    counts_in,
    counts_out,
    table_v,
    table_s,
    order_v,
    order_s,
    res_sem,
    dens_sem,
    cols_send,
    cols_recv,
    rows_send,
    rows_recv,
    counts_send,
    counts_recv,
    move_send,
    move_recv,
    table_sem,
):
    my_row = lax.axis_index("rows")
    my_col = lax.axis_index("cols")

    def chunk_copy(src, dst, sem, c):
        part = pl.ds(c * CHUNK, CHUNK)
        return pltpu.make_async_copy(src.at[:, part], dst.at[:, part], sem.at[c])

    small = [
        pltpu.make_async_copy(owner_hbm, owner_row, table_sem.at[2]),
        pltpu.make_async_copy(owner_hbm, owner, table_sem.at[3]),
        pltpu.make_async_copy(pairs_hbm, pairs, table_sem.at[4]),
    ]
    for copy in small:
        copy.start()
    for c in range(N_CHUNKS):
        chunk_copy(res_hbm, res, res_sem, c).start()

    row_peers = [lax.rem(my_row + o, n_rows) for o in range(1, n_rows)]
    col_peers = [lax.rem(my_col + o, n_cols) for o in range(1, n_cols)]

    barrier = pltpu.get_barrier_semaphore()
    for r in row_peers:
        pl.semaphore_signal(barrier, inc=1, device_id={"rows": r}, device_id_type=MESH)
    for c in col_peers:
        pl.semaphore_signal(barrier, inc=1, device_id={"cols": c}, device_id_type=MESH)

    for copy in small:
        copy.wait()

    acc[...] = jnp.zeros_like(acc)

    def weight_of(s):
        live = owner[0, s] >= 0
        return jnp.where(live, jnp.where(pairs[0, s] == pairs[1, s], 1.0, 2.0), 0.0)

    def gram_slot(s):
        weight = weight_of(s)
        parts = [
            res[:, s, pl.ds(g * GROUP, GROUP), :].reshape(STACK, BLOCK)
            for g in range(BLOCK // GROUP)
        ]
        left = jnp.concatenate(parts, axis=1)
        return left, left * weight.astype(jnp.bfloat16)

    def gram_chunk(c, carry):
        chunk_copy(res_hbm, res, res_sem, c).wait()
        chunk_copy(dens_hbm, dens, dens_sem, c).start()
        pieces = [gram_slot(c * CHUNK + j) for j in range(CHUNK)]
        left = jnp.concatenate([p[0] for p in pieces], axis=1)
        right = jnp.concatenate([p[1] for p in pieces], axis=1)
        acc[...] += lax.dot_general(
            left, right, (((1,), (1,)), ((), ())), preferred_element_type=jnp.float32
        )
        return carry

    lax.fori_loop(0, N_CHUNKS, gram_chunk, 0)

    x_down = lax.broadcasted_iota(jnp.int32, (STACK, STACK), 0)
    x_across = lax.broadcasted_iota(jnp.int32, (STACK, STACK), 1)
    same_x = lax.rem(x_down, GROUP) == lax.rem(x_across, GROUP)
    diag = jnp.where(same_x, acc[...], 0.0).reshape(HIST, GROUP, STACK)
    by_iterate = jnp.sum(diag, axis=1)
    seg = lax.broadcasted_iota(jnp.int32, (HIST, STACK), 1) // GROUP
    i_at = lax.broadcasted_iota(jnp.int32, (HIST, BLOCK), 0)
    lane_at = lax.broadcasted_iota(jnp.int32, (HIST, BLOCK), 1)
    packed = jnp.zeros((HIST, BLOCK), jnp.float32)
    for k in range(HIST):
        entry = jnp.sum(jnp.where(seg == k, by_iterate, 0.0), axis=1, keepdims=True)
        packed = jnp.where(lane_at == i_at * 8 + k, entry, packed)
    row = jnp.sum(packed, axis=0, keepdims=True)

    pl.semaphore_wait(barrier, n_rows + n_cols - 2)

    cols_out[...] = row
    cols_in[my_col] = row

    def cols_copy(peer, slot):
        return pltpu.make_async_remote_copy(
            src_ref=cols_out,
            dst_ref=cols_in.at[slot],
            send_sem=cols_send.at[peer],
            recv_sem=cols_recv.at[slot],
            device_id={"cols": peer},
            device_id_type=MESH,
        )

    def rows_copy(peer, slot):
        return pltpu.make_async_remote_copy(
            src_ref=rows_out,
            dst_ref=rows_in.at[slot],
            send_sem=rows_send.at[peer],
            recv_sem=rows_recv.at[slot],
            device_id={"rows": peer},
            device_id_type=MESH,
        )

    def counts_copy(peer, slot):
        return pltpu.make_async_remote_copy(
            src_ref=counts_out,
            dst_ref=counts_in.at[slot],
            send_sem=counts_send.at[peer],
            recv_sem=counts_recv.at[slot],
            device_id={"rows": peer},
            device_id_type=MESH,
        )

    def move_copy(peer, slot):
        return pltpu.make_async_remote_copy(
            src_ref=outgoing.at[peer],
            dst_ref=arrived.at[pl.ds(slot * CAP, CAP)],
            send_sem=move_send.at[peer],
            recv_sem=move_recv.at[slot],
            device_id={"rows": peer},
            device_id_type=MESH,
        )

    for c in col_peers:
        cols_copy(c, my_col).start()
    own = jnp.broadcast_to(owner_row[...], (HELD, HELD))
    down = lax.broadcasted_iota(jnp.int32, (HELD, HELD), 0)
    across = lax.broadcasted_iota(jnp.int32, (HELD, HELD), 1)
    own_down = jnp.sum(jnp.where(down == across, own, 0), axis=1, keepdims=True)
    same_before = (own == own_down) & (across < down)
    rank_down = jnp.sum(jnp.where(same_before, 1, 0), axis=1, keepdims=True)
    place_down = jnp.where(own_down >= 0, own_down * CAP + rank_down, -1)
    table_v[...] = jnp.sum(jnp.where(place_down == across, down, 0), axis=0, keepdims=True)
    lanes = lax.broadcasted_iota(jnp.int32, (HELD, BLOCK), 1)
    counts_out[...] = jnp.sum(jnp.where(own_down == lanes, 1, 0), axis=0, keepdims=True)
    table_copy = pltpu.make_async_copy(table_v, table_s, table_sem.at[0])
    table_copy.start()

    counts_in[my_row] = counts_out[...]
    for r in row_peers:
        counts_copy(r, my_row).start()
    for c in col_peers:
        cols_copy(c, c).wait_recv()
    row = jnp.sum(cols_in[...], axis=0)
    rows_out[...] = row
    rows_in[my_row] = row
    for r in row_peers:
        rows_copy(r, my_row).start()
    for c in range(N_CHUNKS):
        chunk_copy(dens_hbm, dens, dens_sem, c).wait()
    table_copy.wait()
    for r in row_peers:
        rows_copy(r, r).wait_recv()
    total = jnp.sum(rows_in[...], axis=0)

    def spread(i, k):
        return jnp.broadcast_to(total[:, i * 8 + k : i * 8 + k + 1], (8, BLOCK))

    a = {(i, k): spread(i, k) for i in range(HIST) for k in range(i, HIST)}
    b = [jnp.ones((8, BLOCK), jnp.float32) for _ in range(HIST)]
    for j in range(HIST):
        for i in range(j + 1, HIST):
            factor = a[j, i] / a[j, j]
            for k in range(i, HIST):
                a[i, k] = a[i, k] - factor * a[j, k]
            b[i] = b[i] - factor * b[j]
    solved = [None] * HIST
    for j in reversed(range(HIST)):
        inner = b[j]
        for k in range(j + 1, HIST):
            inner = inner - a[j, k] * solved[k]
        solved[j] = inner / a[j, j]
    norm = functools.reduce(lambda p, q: p + q, solved)
    coef = [s / norm for s in solved]
    lane = lax.broadcasted_iota(jnp.int32, (8, BLOCK), 1)
    shown = jnp.zeros((8, BLOCK), jnp.float32)
    for i in range(HIST):
        shown = jnp.where(lane == i, coef[i], shown)
    coef_out[...] = shown[0:1, 0:HIST]

    coef_d = [c[0:1, :] for c in coef]
    coef_r = [c[0:1, :] * mix_weight for c in coef]

    def blend(q, k):
        slot = table_s[0, q * CAP + k]
        running = None
        for i in range(HIST):
            term = coef_d[i] * dens[i, slot].astype(jnp.float32)
            running = term if running is None else running + term
            running = running + coef_r[i] * res[i, slot].astype(jnp.float32)
        return running.astype(jnp.bfloat16)

    def send_step(o, carry):
        code = SEND_ORDER[-1]
        for t, value in enumerate(SEND_ORDER[:-1]):
            code = jnp.where(o == t, value, code)
        q = lax.rem(my_row // 4 + code // 4, 4) * 4 + lax.rem(my_row + code, 4)
        for k in range(CAP):
            outgoing[q, k] = blend(q, k)
        move_copy(q, my_row).start()
        return carry

    lax.fori_loop(0, len(SEND_ORDER), send_step, 0)
    for k in range(CAP):
        arrived[my_row * CAP + k] = blend(my_row, k)

    for r in row_peers:
        counts_copy(r, r).wait_recv()
    counts = counts_in[...].reshape(n_rows, BLOCK)
    lanes = lax.broadcasted_iota(jnp.int32, (n_rows, BLOCK), 1)
    count_down = jnp.sum(jnp.where(lanes == my_row, counts, 0), axis=1, keepdims=True)
    row_down = lax.broadcasted_iota(jnp.int32, (n_rows, BLOCK), 0)
    count_across = jnp.sum(
        jnp.where(lanes == row_down, count_down, 0), axis=0, keepdims=True
    )
    upto_down = jnp.sum(
        jnp.where(lanes <= row_down, count_across, 0), axis=1, keepdims=True
    )
    skipped = jnp.sum(
        jnp.where(upto_down <= lanes, CAP - count_down, 0), axis=0, keepdims=True
    )
    place = lax.broadcasted_iota(jnp.int32, (1, BLOCK), 1)
    order_v[...] = jnp.minimum(place + skipped, n_rows * CAP - 1)
    order_copy = pltpu.make_async_copy(order_v, order_s, table_sem.at[1])
    order_copy.start()
    order_copy.wait()

    for r in row_peers:
        move_copy(r, r).wait_recv()

    def keep(p, carry):
        for j in range(8):
            owned[p * 8 + j] = arrived[order_s[0, p * 8 + j]]
        return carry

    lax.fori_loop(0, OWNED // 8, keep, 0)

    for c in col_peers:
        cols_copy(c, my_col).wait_send()
    for r in row_peers:
        counts_copy(r, my_row).wait_send()
        rows_copy(r, my_row).wait_send()
        move_copy(r, my_row).wait_send()


def put_out(owned, coef, owned_out, coef_out, sem):
    copies = [
        pltpu.make_async_copy(owned, owned_out, sem.at[0]),
        pltpu.make_async_copy(coef, coef_out, sem.at[1]),
    ]
    for copy in copies:
        copy.start()
    for copy in copies:
        copy.wait()


def solution(mesh):
    n_rows, n_cols = mesh.shape["rows"], mesh.shape["cols"]

    def on_device(densities, residuals, block_pairs, new_owner):
        vmem = pltpu.VMEM
        dma = pltpu.SemaphoreType.DMA
        owned, coef = pl.pallas_call(
            functools.partial(kernel, n_rows, n_cols),
            out_shape=(
                jax.ShapeDtypeStruct((OWNED, BLOCK, BLOCK), jnp.bfloat16),
                jax.ShapeDtypeStruct((1, HIST), jnp.float32),
            ),
            in_specs=[
                pl.BlockSpec(memory_space=pl.ANY),
                pl.BlockSpec(memory_space=pl.ANY),
                pl.BlockSpec(memory_space=pltpu.HBM),
                pl.BlockSpec(memory_space=pltpu.HBM),
            ],
            out_specs=(
                pl.BlockSpec(memory_space=pltpu.VMEM),
                pl.BlockSpec(memory_space=pltpu.VMEM),
            ),
            scratch_shapes=[
                pltpu.SMEM((2, HELD), jnp.int32),
                pltpu.SMEM((1, HELD), jnp.int32),
                vmem((1, HELD), jnp.int32),
                vmem((HIST, HELD, BLOCK, BLOCK), jnp.bfloat16),
                vmem((HIST, HELD, BLOCK, BLOCK), jnp.bfloat16),
                vmem((STACK, STACK), jnp.float32),
                vmem((n_rows, CAP, BLOCK, BLOCK), jnp.bfloat16),
                vmem((n_rows * CAP, BLOCK, BLOCK), jnp.bfloat16),
                vmem((n_cols, 1, BLOCK), jnp.float32),
                vmem((n_rows, 1, BLOCK), jnp.float32),
                vmem((1, BLOCK), jnp.float32),
                vmem((1, BLOCK), jnp.float32),
                vmem((n_rows, 1, BLOCK), jnp.int32),
                vmem((1, BLOCK), jnp.int32),
                vmem((1, HELD), jnp.int32),
                pltpu.SMEM((1, HELD), jnp.int32),
                vmem((1, BLOCK), jnp.int32),
                pltpu.SMEM((1, BLOCK), jnp.int32),
                dma((N_CHUNKS,)),
                dma((N_CHUNKS,)),
                dma((n_cols,)),
                dma((n_cols,)),
                dma((n_rows,)),
                dma((n_rows,)),
                dma((n_rows,)),
                dma((n_rows,)),
                dma((n_rows,)),
                dma((n_rows,)),
                dma((5,)),
            ],
            compiler_params=pltpu.CompilerParams(
                collective_id=0, has_side_effects=True, vmem_limit_bytes=48 * 1024 * 1024
            ),
        )(
            densities,
            residuals,
            pltpu.with_memory_space_constraint(block_pairs, pltpu.HBM),
            pltpu.with_memory_space_constraint(new_owner.reshape(1, HELD), pltpu.HBM),
        )
        owned, coef = pl.pallas_call(
            put_out,
            out_shape=(
                jax.ShapeDtypeStruct((OWNED, BLOCK, BLOCK), jnp.bfloat16),
                jax.ShapeDtypeStruct((1, HIST), jnp.float32),
            ),
            in_specs=[pl.BlockSpec(memory_space=pltpu.VMEM)] * 2,
            out_specs=(pl.BlockSpec(memory_space=pltpu.HBM),) * 2,
            scratch_shapes=[dma((2,))],
            compiler_params=pltpu.CompilerParams(vmem_limit_bytes=2 * 1024 * 1024),
        )(owned, coef)
        return owned, coef.reshape(HIST)

    placed = P(None, ("rows", "cols"), None, None)
    return jax.shard_map(
        on_device,
        mesh=mesh,
        in_specs=(placed, placed, P(None, ("rows", "cols")), P(("rows", "cols"))),
        out_specs=(P(("rows", "cols"), None, None), P()),
        check_vma=False,
    )
```

```python
import functools

import jax
import jax.numpy as jnp
from jax import lax
from jax.experimental import pallas as pl
from jax.experimental.pallas import tpu as pltpu
from jax.sharding import PartitionSpec as P

MESH = pl.DeviceIdType.MESH

HIST = 6
HELD = 64
OWNED = 32
BLOCK = 128
CAP = 4
CHUNK = 16
N_CHUNKS = HELD // CHUNK
GROUP = 16
STACK = HIST * GROUP
SEND_ORDER = [10, 6, 14, 9, 11, 2, 5, 15, 7, 13, 8, 1, 3, 4, 12]

COL_ORDER = [4, 3, 5, 2, 6, 1, 7]

mix_weight = 0.3


def kernel(
    n_rows,
    n_cols,
    dens_hbm,
    res_hbm,
    pairs_hbm,
    owner_hbm,
    owned,
    coef_out,
    pairs,
    owner,
    owner_row,
    dens,
    res,
    acc,
    outgoing,
    arrived,
    cols_in,
    rows_in,
    cols_out,
    rows_out,
    counts_in,
    counts_out,
    table_v,
    table_s,
    order_v,
    order_s,
    res_sem,
    dens_sem,
    cols_send,
    cols_recv,
    rows_send,
    rows_recv,
    counts_send,
    counts_recv,
    move_send,
    move_recv,
    table_sem,
):
    my_row = lax.axis_index("rows")
    my_col = lax.axis_index("cols")

    def chunk_copy(src, dst, sem, c):
        part = pl.ds(c * CHUNK, CHUNK)
        return pltpu.make_async_copy(src.at[:, part], dst.at[:, part], sem.at[c])

    small = [
        pltpu.make_async_copy(owner_hbm, owner_row, table_sem.at[2]),
        pltpu.make_async_copy(owner_hbm, owner, table_sem.at[3]),
        pltpu.make_async_copy(pairs_hbm, pairs, table_sem.at[4]),
    ]
    for copy in small:
        copy.start()
    for c in range(N_CHUNKS):
        chunk_copy(res_hbm, res, res_sem, c).start()

    row_peers = [
        lax.rem(my_row // 4 + code // 4, 4) * 4 + lax.rem(my_row + code, 4) for code in SEND_ORDER
    ]
    col_peers = [lax.rem(my_col + o, n_cols) for o in COL_ORDER]

    barrier = pltpu.get_barrier_semaphore()
    for r in row_peers:
        pl.semaphore_signal(barrier, inc=1, device_id={"rows": r}, device_id_type=MESH)
    for c in col_peers:
        pl.semaphore_signal(barrier, inc=1, device_id={"cols": c}, device_id_type=MESH)

    for copy in small:
        copy.wait()

    acc[...] = jnp.zeros_like(acc)

    def weight_of(s):
        live = owner[0, s] >= 0
        return jnp.where(live, jnp.where(pairs[0, s] == pairs[1, s], 1.0, 2.0), 0.0)

    def gram_slot(s):
        weight = weight_of(s)
        parts = [
            res[:, s, pl.ds(g * GROUP, GROUP), :].reshape(STACK, BLOCK)
            for g in range(BLOCK // GROUP)
        ]
        left = jnp.concatenate(parts, axis=1)
        return left, left * weight.astype(jnp.bfloat16)

    def gram_chunk(c, carry):
        chunk_copy(res_hbm, res, res_sem, c).wait()
        chunk_copy(dens_hbm, dens, dens_sem, c).start()
        for h in range(2):
            pieces = [gram_slot(c * CHUNK + h * (CHUNK // 2) + j) for j in range(CHUNK // 2)]
            left = jnp.concatenate([p[0] for p in pieces], axis=1)
            right = jnp.concatenate([p[1] for p in pieces], axis=1)
            acc[h] += lax.dot_general(
                left, right, (((1,), (1,)), ((), ())), preferred_element_type=jnp.float32
            )
        return carry

    lax.fori_loop(0, N_CHUNKS, gram_chunk, 0)

    x_down = lax.broadcasted_iota(jnp.int32, (STACK, STACK), 0)
    x_across = lax.broadcasted_iota(jnp.int32, (STACK, STACK), 1)
    same_x = lax.rem(x_down, GROUP) == lax.rem(x_across, GROUP)
    diag = jnp.where(same_x, jnp.sum(acc[...], axis=0), 0.0).reshape(HIST, GROUP, STACK)
    by_iterate = jnp.sum(diag, axis=1)
    seg = lax.broadcasted_iota(jnp.int32, (HIST, STACK), 1) // GROUP
    i_at = lax.broadcasted_iota(jnp.int32, (HIST, BLOCK), 0)
    lane_at = lax.broadcasted_iota(jnp.int32, (HIST, BLOCK), 1)
    packed = jnp.zeros((HIST, BLOCK), jnp.float32)
    for k in range(HIST):
        entry = jnp.sum(jnp.where(seg == k, by_iterate, 0.0), axis=1, keepdims=True)
        packed = jnp.where(lane_at == i_at * 8 + k, entry, packed)
    row = jnp.sum(packed, axis=0, keepdims=True)

    pl.semaphore_wait(barrier, n_rows + n_cols - 2)

    cols_out[...] = row
    cols_in[my_col] = row

    def cols_copy(peer, slot):
        return pltpu.make_async_remote_copy(
            src_ref=cols_out,
            dst_ref=cols_in.at[slot],
            send_sem=cols_send.at[peer],
            recv_sem=cols_recv.at[slot],
            device_id={"cols": peer},
            device_id_type=MESH,
        )

    def rows_copy(peer, slot):
        return pltpu.make_async_remote_copy(
            src_ref=rows_out,
            dst_ref=rows_in.at[slot],
            send_sem=rows_send.at[peer],
            recv_sem=rows_recv.at[slot],
            device_id={"rows": peer},
            device_id_type=MESH,
        )

    def counts_copy(peer, slot):
        return pltpu.make_async_remote_copy(
            src_ref=counts_out,
            dst_ref=counts_in.at[slot],
            send_sem=counts_send.at[peer],
            recv_sem=counts_recv.at[slot],
            device_id={"rows": peer},
            device_id_type=MESH,
        )

    def move_copy(peer, slot):
        return pltpu.make_async_remote_copy(
            src_ref=outgoing.at[peer],
            dst_ref=arrived.at[pl.ds(slot * CAP, CAP)],
            send_sem=move_send.at[peer],
            recv_sem=move_recv.at[slot],
            device_id={"rows": peer},
            device_id_type=MESH,
        )

    for c in col_peers:
        cols_copy(c, my_col).start()
    own = jnp.broadcast_to(owner_row[...], (HELD, HELD))
    down = lax.broadcasted_iota(jnp.int32, (HELD, HELD), 0)
    across = lax.broadcasted_iota(jnp.int32, (HELD, HELD), 1)
    own_down = jnp.sum(jnp.where(down == across, own, 0), axis=1, keepdims=True)
    same_before = (own == own_down) & (across < down)
    rank_down = jnp.sum(jnp.where(same_before, 1, 0), axis=1, keepdims=True)
    place_down = jnp.where(own_down >= 0, own_down * CAP + rank_down, -1)
    table_v[...] = jnp.sum(jnp.where(place_down == across, down, 0), axis=0, keepdims=True)
    lanes = lax.broadcasted_iota(jnp.int32, (HELD, BLOCK), 1)
    counts_out[...] = jnp.sum(jnp.where(own_down == lanes, 1, 0), axis=0, keepdims=True)
    table_copy = pltpu.make_async_copy(table_v, table_s, table_sem.at[0])
    table_copy.start()

    counts_in[my_row] = counts_out[...]
    for r in row_peers:
        counts_copy(r, my_row).start()
    for c in col_peers:
        cols_copy(c, c).wait_recv()
    row = jnp.sum(cols_in[...], axis=0)
    rows_out[...] = row
    rows_in[my_row] = row
    for r in row_peers:
        rows_copy(r, my_row).start()
    for c in range(N_CHUNKS):
        chunk_copy(dens_hbm, dens, dens_sem, c).wait()
    table_copy.wait()
    for r in row_peers:
        rows_copy(r, r).wait_recv()
    total = jnp.sum(rows_in[...], axis=0)

    def spread(i, k):
        return jnp.broadcast_to(total[:, i * 8 + k : i * 8 + k + 1], (8, BLOCK))

    a = {(i, k): spread(i, k) for i in range(HIST) for k in range(i, HIST)}
    b = [jnp.ones((8, BLOCK), jnp.float32) for _ in range(HIST)]
    for j in range(HIST):
        for i in range(j + 1, HIST):
            factor = a[j, i] / a[j, j]
            for k in range(i, HIST):
                a[i, k] = a[i, k] - factor * a[j, k]
            b[i] = b[i] - factor * b[j]
    solved = [None] * HIST
    for j in reversed(range(HIST)):
        inner = b[j]
        for k in range(j + 1, HIST):
            inner = inner - a[j, k] * solved[k]
        solved[j] = inner / a[j, j]
    norm = functools.reduce(lambda p, q: p + q, solved)
    coef = [s / norm for s in solved]
    lane = lax.broadcasted_iota(jnp.int32, (8, BLOCK), 1)
    shown = jnp.zeros((8, BLOCK), jnp.float32)
    for i in range(HIST):
        shown = jnp.where(lane == i, coef[i], shown)
    coef_out[...] = shown[0:1, 0:HIST]

    coef_d = [c[0:1, :] for c in coef]
    coef_r = [c[0:1, :] * mix_weight for c in coef]

    def blend(q, k):
        slot = table_s[0, q * CAP + k]
        running = None
        for i in range(HIST):
            term = coef_d[i] * dens[i, slot].astype(jnp.float32)
            running = term if running is None else running + term
            running = running + coef_r[i] * res[i, slot].astype(jnp.float32)
        return running.astype(jnp.bfloat16)

    def send_step(o, carry):
        code = SEND_ORDER[-1]
        for t, value in enumerate(SEND_ORDER[:-1]):
            code = jnp.where(o == t, value, code)
        q = lax.rem(my_row // 4 + code // 4, 4) * 4 + lax.rem(my_row + code, 4)
        for k in range(CAP):
            outgoing[q, k] = blend(q, k)
        move_copy(q, my_row).start()
        return carry

    lax.fori_loop(0, len(SEND_ORDER), send_step, 0)
    for k in range(CAP):
        arrived[my_row * CAP + k] = blend(my_row, k)

    for r in row_peers:
        counts_copy(r, r).wait_recv()
    counts = counts_in[...].reshape(n_rows, BLOCK)
    lanes = lax.broadcasted_iota(jnp.int32, (n_rows, BLOCK), 1)
    count_down = jnp.sum(jnp.where(lanes == my_row, counts, 0), axis=1, keepdims=True)
    row_down = lax.broadcasted_iota(jnp.int32, (n_rows, BLOCK), 0)
    count_across = jnp.sum(
        jnp.where(lanes == row_down, count_down, 0), axis=0, keepdims=True
    )
    upto_down = jnp.sum(
        jnp.where(lanes <= row_down, count_across, 0), axis=1, keepdims=True
    )
    skipped = jnp.sum(
        jnp.where(upto_down <= lanes, CAP - count_down, 0), axis=0, keepdims=True
    )
    place = lax.broadcasted_iota(jnp.int32, (1, BLOCK), 1)
    order_v[...] = jnp.minimum(place + skipped, n_rows * CAP - 1)
    order_copy = pltpu.make_async_copy(order_v, order_s, table_sem.at[1])
    order_copy.start()
    order_copy.wait()

    for r in row_peers:
        move_copy(r, r).wait_recv()

    def keep(p, carry):
        for j in range(8):
            owned[p * 8 + j] = arrived[order_s[0, p * 8 + j]]
        return carry

    lax.fori_loop(0, OWNED // 8, keep, 0)

    for c in col_peers:
        cols_copy(c, my_col).wait_send()
    for r in row_peers:
        counts_copy(r, my_row).wait_send()
        rows_copy(r, my_row).wait_send()
        move_copy(r, my_row).wait_send()


def put_out(owned, coef, owned_out, coef_out, sem):
    copies = [
        pltpu.make_async_copy(owned, owned_out, sem.at[0]),
        pltpu.make_async_copy(coef, coef_out, sem.at[1]),
    ]
    for copy in copies:
        copy.start()
    for copy in copies:
        copy.wait()


def solution(mesh):
    n_rows, n_cols = mesh.shape["rows"], mesh.shape["cols"]

    def on_device(densities, residuals, block_pairs, new_owner):
        vmem = pltpu.VMEM
        dma = pltpu.SemaphoreType.DMA
        owned, coef = pl.pallas_call(
            functools.partial(kernel, n_rows, n_cols),
            out_shape=(
                jax.ShapeDtypeStruct((OWNED, BLOCK, BLOCK), jnp.bfloat16),
                jax.ShapeDtypeStruct((1, HIST), jnp.float32),
            ),
            in_specs=[
                pl.BlockSpec(memory_space=pl.ANY),
                pl.BlockSpec(memory_space=pl.ANY),
                pl.BlockSpec(memory_space=pltpu.HBM),
                pl.BlockSpec(memory_space=pltpu.HBM),
            ],
            out_specs=(
                pl.BlockSpec(memory_space=pltpu.VMEM),
                pl.BlockSpec(memory_space=pltpu.VMEM),
            ),
            scratch_shapes=[
                pltpu.SMEM((2, HELD), jnp.int32),
                pltpu.SMEM((1, HELD), jnp.int32),
                vmem((1, HELD), jnp.int32),
                vmem((HIST, HELD, BLOCK, BLOCK), jnp.bfloat16),
                vmem((HIST, HELD, BLOCK, BLOCK), jnp.bfloat16),
                vmem((2, STACK, STACK), jnp.float32),
                vmem((n_rows, CAP, BLOCK, BLOCK), jnp.bfloat16),
                vmem((n_rows * CAP, BLOCK, BLOCK), jnp.bfloat16),
                vmem((n_cols, 1, BLOCK), jnp.float32),
                vmem((n_rows, 1, BLOCK), jnp.float32),
                vmem((1, BLOCK), jnp.float32),
                vmem((1, BLOCK), jnp.float32),
                vmem((n_rows, 1, BLOCK), jnp.int32),
                vmem((1, BLOCK), jnp.int32),
                vmem((1, HELD), jnp.int32),
                pltpu.SMEM((1, HELD), jnp.int32),
                vmem((1, BLOCK), jnp.int32),
                pltpu.SMEM((1, BLOCK), jnp.int32),
                dma((N_CHUNKS,)),
                dma((N_CHUNKS,)),
                dma((n_cols,)),
                dma((n_cols,)),
                dma((n_rows,)),
                dma((n_rows,)),
                dma((n_rows,)),
                dma((n_rows,)),
                dma((n_rows,)),
                dma((n_rows,)),
                dma((5,)),
            ],
            compiler_params=pltpu.CompilerParams(
                collective_id=0, has_side_effects=True, vmem_limit_bytes=48 * 1024 * 1024
            ),
        )(
            densities,
            residuals,
            pltpu.with_memory_space_constraint(block_pairs, pltpu.HBM),
            pltpu.with_memory_space_constraint(new_owner.reshape(1, HELD), pltpu.HBM),
        )
        owned, coef = pl.pallas_call(
            put_out,
            out_shape=(
                jax.ShapeDtypeStruct((OWNED, BLOCK, BLOCK), jnp.bfloat16),
                jax.ShapeDtypeStruct((1, HIST), jnp.float32),
            ),
            in_specs=[pl.BlockSpec(memory_space=pltpu.VMEM)] * 2,
            out_specs=(pl.BlockSpec(memory_space=pltpu.HBM),) * 2,
            scratch_shapes=[dma((2,))],
            compiler_params=pltpu.CompilerParams(vmem_limit_bytes=2 * 1024 * 1024),
        )(owned, coef)
        return owned, coef.reshape(HIST)

    placed = P(None, ("rows", "cols"), None, None)
    return jax.shard_map(
        on_device,
        mesh=mesh,
        in_specs=(placed, placed, P(None, ("rows", "cols")), P(("rows", "cols"))),
        out_specs=(P(("rows", "cols"), None, None), P()),
        check_vma=False,
    )
```

```python
import functools

import jax
import jax.numpy as jnp
from jax import lax
from jax.experimental import pallas as pl
from jax.experimental.pallas import tpu as pltpu
from jax.sharding import PartitionSpec as P

MESH = pl.DeviceIdType.MESH

HIST = 6
HELD = 64
OWNED = 32
BLOCK = 128
CAP = 4
CHUNK = 16
N_CHUNKS = HELD // CHUNK
GROUP = 16
STACK = HIST * GROUP
SEND_ORDER = [10, 6, 14, 9, 11, 2, 5, 15, 7, 13, 8, 1, 3, 4, 12]

COL_ORDER = [4, 3, 5, 2, 6, 1, 7]

mix_weight = 0.3


def kernel(
    n_rows,
    n_cols,
    dens_hbm,
    res_hbm,
    pairs_hbm,
    owner_hbm,
    owned,
    coef_out,
    pairs,
    owner,
    owner_row,
    dens,
    res,
    acc,
    outgoing,
    arrived,
    cols_in,
    rows_in,
    cols_out,
    rows_out,
    counts_in,
    counts_out,
    table_v,
    table_s,
    order_v,
    order_s,
    res_sem,
    dens_sem,
    cols_send,
    cols_recv,
    rows_send,
    rows_recv,
    counts_send,
    counts_recv,
    move_send,
    move_recv,
    table_sem,
):
    my_row = lax.axis_index("rows")
    my_col = lax.axis_index("cols")

    def chunk_copy(src, dst, sem, c):
        part = pl.ds(c * CHUNK, CHUNK)
        return pltpu.make_async_copy(src.at[:, part], dst.at[:, part], sem.at[c])

    small = [
        pltpu.make_async_copy(owner_hbm, owner_row, table_sem.at[2]),
        pltpu.make_async_copy(owner_hbm, owner, table_sem.at[3]),
        pltpu.make_async_copy(pairs_hbm, pairs, table_sem.at[4]),
    ]
    for copy in small:
        copy.start()
    for c in range(N_CHUNKS):
        chunk_copy(res_hbm, res, res_sem, c).start()

    row_peers = [
        lax.rem(my_row // 4 + code // 4, 4) * 4 + lax.rem(my_row + code, 4) for code in SEND_ORDER
    ]
    col_peers = [lax.rem(my_col + o, n_cols) for o in COL_ORDER]

    barrier = pltpu.get_barrier_semaphore()
    for r in row_peers:
        pl.semaphore_signal(barrier, inc=1, device_id={"rows": r}, device_id_type=MESH)
    for c in col_peers:
        pl.semaphore_signal(barrier, inc=1, device_id={"cols": c}, device_id_type=MESH)

    for copy in small:
        copy.wait()

    acc[...] = jnp.zeros_like(acc)

    def weight_of(s):
        live = owner[0, s] >= 0
        return jnp.where(live, jnp.where(pairs[0, s] == pairs[1, s], 1.0, 2.0), 0.0)

    def gram_slot(s):
        weight = weight_of(s)
        parts = [
            res[:, s, pl.ds(g * GROUP, GROUP), :].reshape(STACK, BLOCK)
            for g in range(BLOCK // GROUP)
        ]
        left = jnp.concatenate(parts, axis=1)
        return left, left * weight.astype(jnp.bfloat16)

    def gram_chunk(c, carry):
        chunk_copy(res_hbm, res, res_sem, c).wait()
        chunk_copy(dens_hbm, dens, dens_sem, c).start()
        for h in range(1):
            pieces = [gram_slot(c * CHUNK + h * (CHUNK // 1) + j) for j in range(CHUNK // 1)]
            left = jnp.concatenate([p[0] for p in pieces], axis=1)
            right = jnp.concatenate([p[1] for p in pieces], axis=1)
            acc[h] += lax.dot_general(
                left, right, (((1,), (1,)), ((), ())), preferred_element_type=jnp.float32
            )
        return carry

    lax.fori_loop(0, N_CHUNKS, gram_chunk, 0)

    x_down = lax.broadcasted_iota(jnp.int32, (STACK, STACK), 0)
    x_across = lax.broadcasted_iota(jnp.int32, (STACK, STACK), 1)
    same_x = lax.rem(x_down, GROUP) == lax.rem(x_across, GROUP)
    diag = jnp.where(same_x, jnp.sum(acc[...], axis=0), 0.0).reshape(HIST, GROUP, STACK)
    by_iterate = jnp.sum(diag, axis=1)
    seg = lax.broadcasted_iota(jnp.int32, (HIST, STACK), 1) // GROUP
    i_at = lax.broadcasted_iota(jnp.int32, (HIST, BLOCK), 0)
    lane_at = lax.broadcasted_iota(jnp.int32, (HIST, BLOCK), 1)
    packed = jnp.zeros((HIST, BLOCK), jnp.float32)
    for k in range(HIST):
        entry = jnp.sum(jnp.where(seg == k, by_iterate, 0.0), axis=1, keepdims=True)
        packed = jnp.where(lane_at == i_at * 8 + k, entry, packed)
    row = jnp.sum(packed, axis=0, keepdims=True)

    pl.semaphore_wait(barrier, n_rows + n_cols - 2)

    cols_out[...] = row
    cols_in[my_col] = row

    def cols_copy(peer, slot):
        return pltpu.make_async_remote_copy(
            src_ref=cols_out,
            dst_ref=cols_in.at[slot],
            send_sem=cols_send.at[peer],
            recv_sem=cols_recv.at[slot],
            device_id={"cols": peer},
            device_id_type=MESH,
        )

    def rows_copy(peer, slot):
        return pltpu.make_async_remote_copy(
            src_ref=rows_out,
            dst_ref=rows_in.at[slot],
            send_sem=rows_send.at[peer],
            recv_sem=rows_recv.at[slot],
            device_id={"rows": peer},
            device_id_type=MESH,
        )

    def counts_copy(peer, slot):
        return pltpu.make_async_remote_copy(
            src_ref=counts_out,
            dst_ref=counts_in.at[slot],
            send_sem=counts_send.at[peer],
            recv_sem=counts_recv.at[slot],
            device_id={"rows": peer},
            device_id_type=MESH,
        )

    def move_copy(peer, slot):
        return pltpu.make_async_remote_copy(
            src_ref=outgoing.at[peer],
            dst_ref=arrived.at[pl.ds(slot * CAP, CAP)],
            send_sem=move_send.at[peer],
            recv_sem=move_recv.at[slot],
            device_id={"rows": peer},
            device_id_type=MESH,
        )

    for c in col_peers:
        cols_copy(c, my_col).start()
    own = jnp.broadcast_to(owner_row[...], (HELD, HELD))
    down = lax.broadcasted_iota(jnp.int32, (HELD, HELD), 0)
    across = lax.broadcasted_iota(jnp.int32, (HELD, HELD), 1)
    own_down = jnp.sum(jnp.where(down == across, own, 0), axis=1, keepdims=True)
    same_before = (own == own_down) & (across < down)
    rank_down = jnp.sum(jnp.where(same_before, 1, 0), axis=1, keepdims=True)
    place_down = jnp.where(own_down >= 0, own_down * CAP + rank_down, -1)
    table_v[...] = jnp.sum(jnp.where(place_down == across, down, 0), axis=0, keepdims=True)
    lanes = lax.broadcasted_iota(jnp.int32, (HELD, BLOCK), 1)
    counts_out[...] = jnp.sum(jnp.where(own_down == lanes, 1, 0), axis=0, keepdims=True)
    table_copy = pltpu.make_async_copy(table_v, table_s, table_sem.at[0])
    table_copy.start()

    counts_in[my_row] = counts_out[...]
    for r in row_peers:
        counts_copy(r, my_row).start()
    for c in col_peers:
        cols_copy(c, c).wait_recv()
    row = jnp.sum(cols_in[...], axis=0)
    rows_out[...] = row
    rows_in[my_row] = row
    for r in row_peers:
        rows_copy(r, my_row).start()
    for c in range(N_CHUNKS):
        chunk_copy(dens_hbm, dens, dens_sem, c).wait()
    table_copy.wait()
    for r in row_peers:
        rows_copy(r, r).wait_recv()
    total = jnp.sum(rows_in[...], axis=0)

    def spread(i, k):
        return jnp.broadcast_to(total[:, i * 8 + k : i * 8 + k + 1], (8, BLOCK))

    a = {(i, k): spread(i, k) for i in range(HIST) for k in range(i, HIST)}
    b = [jnp.ones((8, BLOCK), jnp.float32) for _ in range(HIST)]
    for j in range(HIST):
        for i in range(j + 1, HIST):
            factor = a[j, i] / a[j, j]
            for k in range(i, HIST):
                a[i, k] = a[i, k] - factor * a[j, k]
            b[i] = b[i] - factor * b[j]
    solved = [None] * HIST
    for j in reversed(range(HIST)):
        inner = b[j]
        for k in range(j + 1, HIST):
            inner = inner - a[j, k] * solved[k]
        solved[j] = inner / a[j, j]
    norm = functools.reduce(lambda p, q: p + q, solved)
    coef = [s / norm for s in solved]
    lane = lax.broadcasted_iota(jnp.int32, (8, BLOCK), 1)
    shown = jnp.zeros((8, BLOCK), jnp.float32)
    for i in range(HIST):
        shown = jnp.where(lane == i, coef[i], shown)
    coef_out[...] = shown[0:1, 0:HIST]

    coef_d = [c[0:1, :] for c in coef]
    coef_r = [c[0:1, :] * mix_weight for c in coef]

    def blend(q, k):
        slot = table_s[0, q * CAP + k]
        running = None
        for i in range(HIST):
            term = coef_d[i] * dens[i, slot].astype(jnp.float32)
            running = term if running is None else running + term
            running = running + coef_r[i] * res[i, slot].astype(jnp.float32)
        return running.astype(jnp.bfloat16)

    def send_step(o, carry):
        code = SEND_ORDER[-1]
        for t, value in enumerate(SEND_ORDER[:-1]):
            code = jnp.where(o == t, value, code)
        q = lax.rem(my_row // 4 + code // 4, 4) * 4 + lax.rem(my_row + code, 4)
        for k in range(CAP):
            outgoing[q, k] = blend(q, k)
        move_copy(q, my_row).start()
        return carry

    lax.fori_loop(0, len(SEND_ORDER), send_step, 0)
    for k in range(CAP):
        arrived[my_row * CAP + k] = blend(my_row, k)

    for r in row_peers:
        counts_copy(r, r).wait_recv()
    counts = counts_in[...].reshape(n_rows, BLOCK)
    lanes = lax.broadcasted_iota(jnp.int32, (n_rows, BLOCK), 1)
    count_down = jnp.sum(jnp.where(lanes == my_row, counts, 0), axis=1, keepdims=True)
    row_down = lax.broadcasted_iota(jnp.int32, (n_rows, BLOCK), 0)
    count_across = jnp.sum(
        jnp.where(lanes == row_down, count_down, 0), axis=0, keepdims=True
    )
    upto_down = jnp.sum(
        jnp.where(lanes <= row_down, count_across, 0), axis=1, keepdims=True
    )
    skipped = jnp.sum(
        jnp.where(upto_down <= lanes, CAP - count_down, 0), axis=0, keepdims=True
    )
    place = lax.broadcasted_iota(jnp.int32, (1, BLOCK), 1)
    order_v[...] = jnp.minimum(place + skipped, n_rows * CAP - 1)
    order_copy = pltpu.make_async_copy(order_v, order_s, table_sem.at[1])
    order_copy.start()
    order_copy.wait()

    for r in row_peers:
        move_copy(r, r).wait_recv()

    def keep(p, carry):
        for j in range(8):
            owned[p * 8 + j] = arrived[order_s[0, p * 8 + j]]
        return carry

    lax.fori_loop(0, OWNED // 8, keep, 0)

    for c in col_peers:
        cols_copy(c, my_col).wait_send()
    for r in row_peers:
        counts_copy(r, my_row).wait_send()
        rows_copy(r, my_row).wait_send()
        move_copy(r, my_row).wait_send()


def put_out(owned, coef, owned_out, coef_out, sem):
    copies = [
        pltpu.make_async_copy(owned, owned_out, sem.at[0]),
        pltpu.make_async_copy(coef, coef_out, sem.at[1]),
    ]
    for copy in copies:
        copy.start()
    for copy in copies:
        copy.wait()


def solution(mesh):
    n_rows, n_cols = mesh.shape["rows"], mesh.shape["cols"]

    def on_device(densities, residuals, block_pairs, new_owner):
        vmem = pltpu.VMEM
        dma = pltpu.SemaphoreType.DMA
        owned, coef = pl.pallas_call(
            functools.partial(kernel, n_rows, n_cols),
            out_shape=(
                jax.ShapeDtypeStruct((OWNED, BLOCK, BLOCK), jnp.bfloat16),
                jax.ShapeDtypeStruct((1, HIST), jnp.float32),
            ),
            in_specs=[
                pl.BlockSpec(memory_space=pl.ANY),
                pl.BlockSpec(memory_space=pl.ANY),
                pl.BlockSpec(memory_space=pltpu.HBM),
                pl.BlockSpec(memory_space=pltpu.HBM),
            ],
            out_specs=(
                pl.BlockSpec(memory_space=pltpu.VMEM),
                pl.BlockSpec(memory_space=pltpu.VMEM),
            ),
            scratch_shapes=[
                pltpu.SMEM((2, HELD), jnp.int32),
                pltpu.SMEM((1, HELD), jnp.int32),
                vmem((1, HELD), jnp.int32),
                vmem((HIST, HELD, BLOCK, BLOCK), jnp.bfloat16),
                vmem((HIST, HELD, BLOCK, BLOCK), jnp.bfloat16),
                vmem((1, STACK, STACK), jnp.float32),
                vmem((n_rows, CAP, BLOCK, BLOCK), jnp.bfloat16),
                vmem((n_rows * CAP, BLOCK, BLOCK), jnp.bfloat16),
                vmem((n_cols, 1, BLOCK), jnp.float32),
                vmem((n_rows, 1, BLOCK), jnp.float32),
                vmem((1, BLOCK), jnp.float32),
                vmem((1, BLOCK), jnp.float32),
                vmem((n_rows, 1, BLOCK), jnp.int32),
                vmem((1, BLOCK), jnp.int32),
                vmem((1, HELD), jnp.int32),
                pltpu.SMEM((1, HELD), jnp.int32),
                vmem((1, BLOCK), jnp.int32),
                pltpu.SMEM((1, BLOCK), jnp.int32),
                dma((N_CHUNKS,)),
                dma((N_CHUNKS,)),
                dma((n_cols,)),
                dma((n_cols,)),
                dma((n_rows,)),
                dma((n_rows,)),
                dma((n_rows,)),
                dma((n_rows,)),
                dma((n_rows,)),
                dma((n_rows,)),
                dma((5,)),
            ],
            compiler_params=pltpu.CompilerParams(
                collective_id=0, has_side_effects=True, vmem_limit_bytes=48 * 1024 * 1024
            ),
        )(
            densities,
            residuals,
            pltpu.with_memory_space_constraint(block_pairs, pltpu.HBM),
            pltpu.with_memory_space_constraint(new_owner.reshape(1, HELD), pltpu.HBM),
        )
        owned, coef = pl.pallas_call(
            put_out,
            out_shape=(
                jax.ShapeDtypeStruct((OWNED, BLOCK, BLOCK), jnp.bfloat16),
                jax.ShapeDtypeStruct((1, HIST), jnp.float32),
            ),
            in_specs=[pl.BlockSpec(memory_space=pltpu.VMEM)] * 2,
            out_specs=(pl.BlockSpec(memory_space=pltpu.HBM),) * 2,
            scratch_shapes=[dma((2,))],
            compiler_params=pltpu.CompilerParams(vmem_limit_bytes=2 * 1024 * 1024),
        )(owned, coef)
        return owned, coef.reshape(HIST)

    placed = P(None, ("rows", "cols"), None, None)
    return jax.shard_map(
        on_device,
        mesh=mesh,
        in_specs=(placed, placed, P(None, ("rows", "cols")), P(("rows", "cols"))),
        out_specs=(P(("rows", "cols"), None, None), P()),
        check_vma=False,
    )
```
